32 devices in a mesh: dp: 32 (over z, y, x, core).
Axes of the slice: x: 2, y: 2, z: 4, core: 2. Of those that a mesh axis runs over, the one named last changes fastest.
Arguments:
- u_norm: bfloat16 [16, 2048, 4096], P(None, 'dp')
- expert_idx: int32 [16, 2048, 2], P(None, 'dp')
- expert_out: bfloat16 [16, 2048, 2, 4096], P(None, 'dp')
- d_out: bfloat16 [16, 2048, 4096], P(None, 'dp')
- w_router: bfloat16 [16, 4096, 16], replicated
Outputs:
- output 1: float32 [], replicated
- output 2: float32 [16, 4096, 16], replicated
- output 3: bfloat16 [16, 2048, 4096], P(None, 'dp')
All inputs are finite; a program needn't handle non-finite values.
Results may differ from the reference program's by a relative error of at most 0.00944661.
Values sent between devices are 32-bit elements.
A program may use at most 1 GiB of HBM per device.

```python
import jax
import jax.numpy as jnp
from jax import lax

LAYERS = 16
GROUP = 32
TOK_DEV = 64
D = 4096
EXPERTS = 16
TOP = 2

TOKENS = GROUP * TOK_DEV
AUX_COEF = 0.02
LOSS_SCALE = 1.0 * TOKENS
DY_SCALE = 0.015 * (TOP / (EXPERTS * TOKENS * D)) ** 0.5


def draw_slots(slot_key):
    expert_ids = jnp.arange(EXPERTS)
    tok_pos = jnp.arange(TOKENS)
    tok_owner = tok_pos // TOK_DEV
    favored = (expert_ids[None, :] == (tok_owner % EXPERTS)[:, None]).astype(jnp.int32)
    weights = 1 + expert_ids[None, :] % 3 + 12 * favored
    tickets = jax.random.randint(slot_key, (LAYERS, TOKENS, EXPERTS), 0, 4096)
    int_score = weights[None] * tickets * EXPERTS + expert_ids
    drawn_ids = lax.top_k(int_score, TOP)[1]
    forced = (tok_pos[:, None] + jnp.arange(TOP)[None, :]) % EXPERTS
    chosen_ids = jnp.where((tok_pos < EXPERTS)[None, :, None], forced[None], drawn_ids)
    return chosen_ids.astype(jnp.int32)


def setup_inputs(seed: int = 0) -> dict:
    base_key = jax.random.key(seed)
    key_list = jax.random.split(base_key, 7)
    global_mean = 0.5 * jax.random.normal(key_list[0], (LAYERS, 1, D), jnp.float32)
    device_mean = 0.5 * jax.random.normal(key_list[1], (LAYERS, GROUP, 1, D), jnp.float32)
    noise_vals = jax.random.normal(key_list[2], (LAYERS, GROUP, TOK_DEV, D), jnp.float32)
    u_vals = (noise_vals + device_mean).reshape(LAYERS, TOKENS, D) + global_mean
    expert_out = jax.random.normal(key_list[4], (LAYERS, TOKENS, TOP, D), jnp.float32)
    d_out = DY_SCALE * jax.random.normal(key_list[5], (LAYERS, TOKENS, D), jnp.float32)
    w_router = jax.random.normal(key_list[6], (LAYERS, D, EXPERTS), jnp.float32) * D ** -0.5
    return {
        'u_norm': u_vals.astype(jnp.bfloat16),
        'expert_idx': draw_slots(key_list[3]),
        'expert_out': expert_out.astype(jnp.bfloat16),
        'd_out': d_out.astype(jnp.bfloat16),
        'w_router': w_router.astype(jnp.bfloat16),
    }


def reference(u_norm, expert_idx, expert_out, d_out, w_router):
    def one_layer(layer_in):
        u_layer, idx_layer, out_layer, dy_layer, w_layer = layer_in
        logits = jnp.dot(u_layer, w_layer, preferred_element_type=jnp.float32)
        slot_dots = jnp.einsum('tkd,td->tk', out_layer.astype(jnp.float32), dy_layer.astype(jnp.float32))
        one_hot = jax.nn.one_hot(idx_layer, EXPERTS, dtype=jnp.float32)
        exp_frac = jnp.sum(one_hot, axis=(0, 1)) / (TOP * TOKENS)

        def loss_of(logit_in):
            prob_vals = jax.nn.softmax(logit_in, axis=-1)
            gate_vals = jax.nn.softmax(jnp.take_along_axis(logit_in, idx_layer, axis=-1), axis=-1)
            main_part = jnp.sum(gate_vals * slot_dots)
            aux_part = EXPERTS * jnp.sum(exp_frac * jnp.mean(prob_vals, axis=0))
            return main_part + AUX_COEF * aux_part

        layer_loss, pull_back = jax.vjp(loss_of, logits)
        d_logits = pull_back(jnp.ones_like(layer_loss) * LOSS_SCALE)[0]
        d_log16 = d_logits.astype(jnp.bfloat16)
        grad_w = jnp.dot(u_layer.T, d_log16, preferred_element_type=jnp.float32)
        grad_u = jnp.dot(d_log16, w_layer.T, preferred_element_type=jnp.float32).astype(jnp.bfloat16)
        return layer_loss, grad_w, grad_u

    layer_losses, d_router, d_norm = lax.map(one_layer, (u_norm, expert_idx, expert_out, d_out, w_router))
    return (jnp.sum(layer_losses), d_router, d_norm)
```

```python
import functools

import jax
import jax.numpy as jnp
from jax import lax
from jax.experimental import pallas as pl
from jax.experimental.pallas import tpu as pltpu
from jax.sharding import PartitionSpec as P

AUX_COEF = 0.02
MESH = pl.DeviceIdType.MESH
F_STRIDE = 72
SLOTS = 4
LAG_B = 11
LAG_R0, LAG_R1, LAG_R2, LAG_R3, LAG_G3, LAG_G2, LAG_G1, LAG_G0 = 1, 2, 2, 3, 3, 2, 2, 2


def ring_kernel(dims, idx_ref, u_hbm, w_hbm, e_hbm, d_hbm, out_ref, g_ref, loss_ref,
                u_all, w_all, e_buf, d_buf, wide, p_all, a_all, part, r0, r1, r2, r3,
                cnt_src, cnt_buf, loss_src, loss_buf, loss_acc, pull_row,
                u_sem, w_sem, e_sem, d_sem, s0, v0, s1, v1, s2, v2, s3, v3, sg3, vg3, sg2, vg2, sg1, vg1, sg0, vg0,
                cs, cv, ls, lv):
    layers, toks, num_exp, depth, top_k, group = dims
    half = depth // 2
    quart = depth // 4
    piece = depth // 16
    me = lax.axis_index('dp')
    core = lax.rem(me, 2)
    px = lax.rem(lax.div(me, 2), 2)
    py = lax.rem(lax.div(me, 4), 2)
    pz = lax.div(me, 8)
    tok_all = toks * group

    def fetch_u(l):
        return (pltpu.make_async_copy(u_hbm.at[l], u_all.at[l], u_sem.at[l]),
                pltpu.make_async_copy(w_hbm.at[l], w_all.at[l], w_sem.at[l]))

    def fetch_e(l):
        slot = lax.rem(l, SLOTS)
        return (pltpu.make_async_copy(e_hbm.at[l], e_buf.at[slot], e_sem.at[slot]),
                pltpu.make_async_copy(d_hbm.at[l], d_buf.at[slot], d_sem.at[slot]))

    for l in range(SLOTS):
        for copy in fetch_u(l) + fetch_e(l):
            copy.start()

    barrier = pltpu.get_barrier_semaphore()

    def greet(p, carry):
        pl.semaphore_signal(barrier, inc=1, device_id=(lax.rem(me + p, group),), device_id_type=MESH)
        return carry
    lax.fori_loop(1, group, greet, 0)

    ids = [idx_ref[:, k, :] for k in range(top_k)]
    rows = []
    for e in range(num_exp):
        hit = jnp.where(ids[0] == e, 1.0, 0.0)
        for k in range(1, top_k):
            hit = hit + jnp.where(ids[k] == e, 1.0, 0.0)
        rows.append(hit)
    hits = jnp.concatenate(rows, axis=0).astype(jnp.bfloat16)
    cnt = lax.dot_general(jnp.ones((8, toks), jnp.bfloat16), hits, (((1,), (1,)), ((), ())),
                          preferred_element_type=jnp.float32)
    cnt_src[...] = cnt[0:1]
    cnt_buf[me] = cnt[0:1]
    loss_acc[...] = jnp.zeros_like(loss_acc)

    pl.semaphore_wait(barrier, group - 1)

    def count_copy(p, dst_slot):
        return pltpu.make_async_remote_copy(
            src_ref=cnt_src, dst_ref=cnt_buf.at[dst_slot], send_sem=cs.at[p], recv_sem=cv.at[p],
            device_id=(lax.rem(me + p, group),), device_id_type=MESH)

    def loss_copy(p, dst_slot):
        return pltpu.make_async_remote_copy(
            src_ref=loss_src, dst_ref=loss_buf.at[dst_slot], send_sem=ls.at[p], recv_sem=lv.at[p],
            device_id=(lax.rem(me + p, group),), device_id_type=MESH)

    def send_counts(p, carry):
        count_copy(p, me).start()
        return carry
    lax.fori_loop(1, group, send_counts, 0)

    def forward(l):
        slot = lax.rem(l, SLOTS)
        for copy in fetch_u(l):
            copy.wait()
        logits = lax.dot_general(w_all[l], u_all[l], (((1,), (1,)), ((), ())), preferred_element_type=jnp.float32)
        for copy in fetch_e(l):
            copy.wait()
        accs = [[], []]
        tiles = depth // 128
        for tb in range(toks // 8):
            for t in range(8):
                tok = tb * 8 + t
                wide[pl.ds(tok * F_STRIDE, 2 * tiles), :] = (
                    e_buf[slot, pl.ds(tok * 2 * tiles, 2 * tiles), :].astype(jnp.float32))
            dy = d_buf[slot, pl.ds(tb * 8 * tiles, 8 * tiles), :].astype(jnp.float32)
            sums = [[None, None], [None, None]]
            for j in range(tiles):
                for k in range(2):
                    ev = wide[pl.ds(tb * 8 * F_STRIDE + 2 * j + k, 8, stride=F_STRIDE), :]
                    prod = ev * dy[8 * j:8 * j + 8]
                    old = sums[k][j % 2]
                    sums[k][j % 2] = prod if old is None else old + prod
            for k in range(2):
                accs[k].append(sums[k][0] + sums[k][1])

        @pl.when(l + SLOTS < layers)
        def _():
            for copy in fetch_u(l + SLOTS) + fetch_e(l + SLOTS):
                copy.start()

        dots = jnp.sum(jnp.concatenate(accs[0] + accs[1], axis=0).T, axis=0, keepdims=True)
        dot0, dot1 = dots[:, :toks], dots[:, toks:]
        row_id = lax.broadcasted_iota(jnp.int32, (num_exp, toks), 0)
        pair = idx_ref[l]
        sel0 = row_id == pair[0:1]
        sel1 = row_id == pair[1:2]
        top = jnp.max(logits, axis=0, keepdims=True)
        ex = jnp.exp(logits - top)
        p_all[l] = ex / jnp.sum(ex, axis=0, keepdims=True)
        c0 = jnp.sum(jnp.where(sel0, logits, 0.0), axis=0, keepdims=True)
        c1 = jnp.sum(jnp.where(sel1, logits, 0.0), axis=0, keepdims=True)
        cm = jnp.maximum(c0, c1)
        x0, x1 = jnp.exp(c0 - cm), jnp.exp(c1 - cm)
        xs = x0 + x1
        g0, g1 = x0 / xs, x1 / xs
        inner = g0 * dot0 + g1 * dot1
        loss_acc[0:1, :] += inner
        scale = float(tok_all)
        dc0 = g0 * (scale * dot0 - scale * inner)
        dc1 = g1 * (scale * dot1 - scale * inner)
        a_all[l] = jnp.where(sel0, dc0, 0.0) + jnp.where(sel1, dc1, 0.0)

    def get_counts():
        def one(p, carry):
            count_copy(p, lax.rem(me + group - p, group)).wait_recv()
            return carry
        lax.fori_loop(1, group, one, 0)
        pull_row[...] = jnp.sum(cnt_buf[...], axis=0) * (AUX_COEF * num_exp / (top_k * tok_all))

    def halves(l):
        odd = lax.rem(l, 2)
        a1 = jnp.where(odd == 0, px, py)
        a2 = jnp.where(odd == 0, py, px)
        step1 = jnp.where(odd == 0, 2, 4)
        step2 = jnp.where(odd == 0, 4, 2)
        peer1 = me + step1 * (1 - 2 * a1)
        peer2 = me + step2 * (1 - 2 * a2)
        return a1, a2, peer1, peer2

    partner = me + 1 - 2 * core

    def lanes(start, size):
        return pl.ds(pl.multiple_of(start, piece), size)

    def remote(src, dst, ss, rs, dev):
        return pltpu.make_async_remote_copy(src_ref=src, dst_ref=dst, send_sem=ss, recv_sem=rs,
                                            device_id=(dev,), device_id_type=MESH)

    def copy_r0(l):
        return [remote(part.at[l, 1 - core], r0.at[l], s0.at[l], v0.at[l], partner)]

    def copy_r1(l):
        a1, a2, peer1, peer2 = halves(l)
        return [remote(part.at[l, core, :, lanes(half * (1 - a1), half)], r1.at[l], s1.at[l], v1.at[l], peer1)]

    def copy_r2(l):
        a1, a2, peer1, peer2 = halves(l)
        return [remote(part.at[l, core, :, lanes(half * a1 + quart * (1 - a2), quart)], r2.at[l], s2.at[l], v2.at[l],
                       peer2)]

    def copy_r3(l):
        a1, a2, peer1, peer2 = halves(l)
        out = []
        for dz in range(1, 4):
            zt = lax.rem(pz + dz, 4)
            out.append(remote(part.at[l, core, :, lanes(half * a1 + quart * a2 + piece * zt, piece)],
                              r3.at[l, dz - 1], s3.at[l, dz - 1], v3.at[l, dz - 1], me + 8 * (zt - pz)))
        return out

    def copy_g3(l, receive=False):
        a1, a2, peer1, peer2 = halves(l)
        out = []
        for dz in range(1, 4):
            zt = lax.rem(pz + dz, 4)
            zo = lax.rem(pz + 4 - dz, 4) if receive else pz
            ref = out_ref.at[l, core, :, lanes(half * a1 + quart * a2 + piece * zo, piece)]
            out.append(remote(ref, ref, sg3.at[l, dz - 1], vg3.at[l, dz - 1], me + 8 * (zt - pz)))
        return out

    def copy_g2(l, receive=False):
        a1, a2, peer1, peer2 = halves(l)
        own = 1 - a2 if receive else a2
        ref = out_ref.at[l, core, :, lanes(half * a1 + quart * own, quart)]
        return [remote(ref, ref, sg2.at[l], vg2.at[l], peer2)]

    def copy_g1(l, receive=False):
        a1, a2, peer1, peer2 = halves(l)
        own = 1 - a1 if receive else a1
        ref = out_ref.at[l, core, :, lanes(half * own, half)]
        return [remote(ref, ref, sg1.at[l], vg1.at[l], peer1)]

    def copy_g0(l, receive=False):
        own = 1 - core if receive else core
        ref = out_ref.at[l, own]
        return [remote(ref, ref, sg0.at[l], vg0.at[l], partner)]

    def start(copies):
        for copy in copies:
            copy.start()

    def landed(copies):
        for copy in copies:
            copy.wait_recv()

    def sent(copies):
        for copy in copies:
            copy.wait_send()

    def backward(l):
        at = lax.broadcasted_iota(jnp.int32, (num_exp, num_exp * layers), 1)
        row = lax.broadcasted_iota(jnp.int32, (num_exp, num_exp * layers), 0)
        pull = jnp.sum(jnp.where(at == layers * row + l, pull_row[...], 0.0), axis=1, keepdims=True)
        prob = p_all[l]
        inner = jnp.sum(prob * pull, axis=0, keepdims=True)
        loss_acc[1:2, :] += inner
        grad = (a_all[l] + prob * (pull - inner)).astype(jnp.bfloat16)
        g_ref[l] = grad
        dw = jnp.dot(grad, u_all[l], preferred_element_type=jnp.float32)
        part[l, 0] = dw[:8]
        part[l, 1] = dw[8:]
        start(copy_r0(l))

        @pl.when(l == layers - 1)
        def _():
            total = loss_acc[0:1, :] + loss_acc[1:2, :] * (1.0 / tok_all)
            mine = jnp.broadcast_to(jnp.sum(total, axis=1, keepdims=True), (1, 128))
            loss_src[...] = mine
            loss_buf[me] = mine

            def send_loss(p, carry):
                loss_copy(p, me).start()
                return carry
            lax.fori_loop(1, group, send_loss, 0)

    def stage_r0(l):
        a1, a2, peer1, peer2 = halves(l)
        landed(copy_r0(l))
        away = lanes(half * (1 - a1), half)
        part[l, core, :, away] += r0[l, :, away]
        start(copy_r1(l))
        keep = lanes(half * a1, half)
        part[l, core, :, keep] += r0[l, :, keep]

    def stage_r1(l):
        a1, a2, peer1, peer2 = halves(l)
        landed(copy_r1(l))
        away = lanes(half * a1 + quart * (1 - a2), quart)
        part[l, core, :, away] += r1[l, :, lanes(quart * (1 - a2), quart)]
        start(copy_r2(l))
        keep = lanes(half * a1 + quart * a2, quart)
        part[l, core, :, keep] += r1[l, :, lanes(quart * a2, quart)]

    def stage_r2(l):
        a1, a2, peer1, peer2 = halves(l)
        landed(copy_r2(l))
        keep = lanes(half * a1 + quart * a2, quart)
        part[l, core, :, keep] += r2[l]
        start(copy_r3(l))

    def stage_r3(l):
        a1, a2, peer1, peer2 = halves(l)
        landed(copy_r3(l))
        keep = lanes(half * a1 + quart * a2 + piece * pz, piece)
        out_ref[l, core, :, keep] = (part[l, core, :, keep] + r3[l, 0]) + (r3[l, 1] + r3[l, 2])
        start(copy_g3(l))

    def stage_g3(l):
        landed(copy_g3(l, True))
        start(copy_g2(l))

    def stage_g2(l):
        landed(copy_g2(l, True))
        start(copy_g1(l))

    def stage_g1(l):
        landed(copy_g1(l, True))
        start(copy_g0(l))

    def stage_g0(l):
        landed(copy_g0(l, True))
        sent(copy_r0(l) + copy_r1(l) + copy_r2(l) + copy_r3(l) + copy_g3(l) + copy_g2(l) + copy_g1(l) + copy_g0(l))

    stages = [(0, forward), (LAG_B, backward)]
    lag = LAG_B
    for add, stage in ((LAG_R0, stage_r0), (LAG_R1, stage_r1), (LAG_R2, stage_r2), (LAG_R3, stage_r3),
                       (LAG_G3, stage_g3), (LAG_G2, stage_g2), (LAG_G1, stage_g1), (LAG_G0, stage_g0)):
        lag += add
        stages.append((lag, stage))

    def step(s, carry):
        @pl.when(s == LAG_B)
        def _():
            get_counts()
        for delay, stage in stages:
            @pl.when(jnp.logical_and(s >= delay, s < delay + layers))
            def _():
                stage(s - delay)
        return carry
    lax.fori_loop(0, layers + lag, step, 0)

    def finish(p, carry):
        count_copy(p, me).wait_send()
        loss_copy(p, me).wait_send()
        loss_copy(p, lax.rem(me + group - p, group)).wait_recv()
        return carry
    lax.fori_loop(1, group, finish, 0)
    loss_ref[...] = jnp.sum(loss_buf[...], axis=0)


def norm_kernel(layers_step, g_ref, w_ref, dr_ref, dn_ref, dr_out, sem):
    step = pl.program_id(0)
    move = pltpu.make_async_copy(dr_ref, dr_out, sem)

    @pl.when(step == 0)
    def _():
        move.start()

    for i in range(layers_step):
        dn_ref[i] = lax.dot_general(g_ref[i], w_ref[i], (((0,), (0,)), ((), ())),
                                    preferred_element_type=jnp.float32).astype(jnp.bfloat16)

    @pl.when(step == pl.num_programs(0) - 1)
    def _():
        move.wait()


def solution(mesh):
    group = mesh.shape['dp']

    def local_step(u_norm, expert_idx, expert_out, d_out, w_router):
        layers, toks, depth = u_norm.shape
        num_exp = w_router.shape[2]
        top_k = expert_idx.shape[2]
        tiles = depth // 128
        idx_t = expert_idx.transpose(0, 2, 1)
        w_t = w_router.transpose(0, 2, 1)
        e_rows = expert_out.reshape(layers, toks, top_k, tiles, 128).transpose(0, 1, 3, 2, 4)
        e_rows = e_rows.reshape(layers, toks * tiles * top_k, 128)
        d_rows = d_out.reshape(layers, toks // 8, 8, tiles, 128).transpose(0, 1, 3, 2, 4)
        d_rows = d_rows.reshape(layers, toks * tiles, 128)
        f32, bf16 = jnp.float32, jnp.bfloat16
        dma = pltpu.SemaphoreType.DMA
        vmem = pl.BlockSpec(memory_space=pltpu.VMEM)
        hbm = pl.BlockSpec(memory_space=pltpu.HBM)
        dims = (layers, toks, num_exp, depth, top_k, group)
        scratch = [
            pltpu.VMEM((layers, toks, depth), bf16), pltpu.VMEM((layers, num_exp, depth), bf16),
            pltpu.VMEM((SLOTS, toks * tiles * top_k, 128), bf16), pltpu.VMEM((SLOTS, toks * tiles, 128), bf16),
            pltpu.VMEM((toks * F_STRIDE, 128), f32),
            pltpu.VMEM((layers, num_exp, toks), f32), pltpu.VMEM((layers, num_exp, toks), f32),
            pltpu.VMEM((layers, 2, 8, depth), f32), pltpu.VMEM((layers, 8, depth), f32),
            pltpu.VMEM((layers, 8, depth // 2), f32), pltpu.VMEM((layers, 8, depth // 4), f32),
            pltpu.VMEM((layers, 3, 8, depth // 16), f32),
            pltpu.VMEM((1, num_exp * layers), f32), pltpu.VMEM((group, 1, num_exp * layers), f32),
            pltpu.VMEM((1, 128), f32), pltpu.VMEM((group, 1, 128), f32), pltpu.VMEM((8, toks), f32),
            pltpu.VMEM((1, num_exp * layers), f32),
            dma((layers,)), dma((layers,)), dma((SLOTS,)), dma((SLOTS,)),
            dma((layers,)), dma((layers,)), dma((layers,)), dma((layers,)), dma((layers,)), dma((layers,)),
            dma((layers, 3)), dma((layers, 3)), dma((layers, 3)), dma((layers, 3)),
            dma((layers,)), dma((layers,)), dma((layers,)), dma((layers,)), dma((layers,)), dma((layers,)),
            dma((group,)), dma((group,)), dma((group,)), dma((group,)),
        ]
        d_router, grads, loss = pl.pallas_call(
            functools.partial(ring_kernel, dims),
            out_shape=(jax.ShapeDtypeStruct((layers, 2, 8, depth), f32),
                       jax.ShapeDtypeStruct((layers, num_exp, toks), bf16),
                       jax.ShapeDtypeStruct((1, 128), f32)),
            in_specs=[vmem, hbm, hbm, hbm, hbm],
            out_specs=(vmem, vmem, vmem),
            scratch_shapes=scratch,
            compiler_params=pltpu.CompilerParams(collective_id=0, has_side_effects=True,
                                                 vmem_limit_bytes=48 * 1024 * 1024),
            name='ring',
        )(idx_t, u_norm, w_t, e_rows, d_rows)

        per = 4
        d_norm, d_router = pl.pallas_call(
            functools.partial(norm_kernel, per),
            grid=(layers // per,),
            out_shape=(jax.ShapeDtypeStruct((layers, toks, depth), bf16),
                       jax.ShapeDtypeStruct((layers, 2, 8, depth), f32)),
            in_specs=[pl.BlockSpec((per, num_exp, toks), lambda i: (i, 0, 0)),
                      pl.BlockSpec((per, num_exp, depth), lambda i: (i, 0, 0)),
                      pl.BlockSpec(memory_space=pl.ANY)],
            out_specs=(pl.BlockSpec((per, toks, depth), lambda i: (i, 0, 0)),
                       pl.BlockSpec(memory_space=pltpu.HBM)),
            scratch_shapes=[dma(())],
            name='norm',
        )(grads, w_t, d_router)
        d_router = d_router.reshape(layers, num_exp, depth).transpose(0, 2, 1)
        return loss[0, 0], d_router, d_norm

    tok_spec = P(None, 'dp', None)
    return jax.shard_map(local_step, mesh=mesh,
                         in_specs=(tok_spec, tok_spec, P(None, 'dp', None, None), tok_spec, P()),
                         out_specs=(P(), P(), tok_spec), check_vma=False)
```

```python
import functools

import jax
import jax.numpy as jnp
from jax import lax
from jax.experimental import pallas as pl
from jax.experimental.pallas import tpu as pltpu
from jax.sharding import PartitionSpec as P

AUX_COEF = 0.02
MESH = pl.DeviceIdType.MESH
F_STRIDE = 73
SLOTS = 6
GREET = 2
BITS = {'c': 1, 'x': 2, 'y': 4, 'p': 8, 'q': 16}
ORDERS = ('xpyq', 'ypxq') * 8
T_START, T_FWD, T_BWD, T_COUNTS = 1.5, 0.85, 0.5, 12.5
T_STAGE = (0.1, 0.08, 0.06, 0.05, 0.05, 0.04, 0.04, 0.04, 0.04, 0.03)
DELAY = {'c': 1.5, 'x': 3.0, 'y': 3.0, 'p': 3.0, 'q': 3.5}
AHEAD = 1.5
PRIO = 3


def plan_order(orders):
    layers = len(orders)
    paths = ['c' + o + o[::-1] + 'c' for o in orders]
    sizes = [2.8 / 2 ** i for i in range(5)]
    sizes = sizes + sizes[::-1]
    link = dict.fromkeys('cxypm', 0.0)
    arrive, plan = {}, []
    now, done_f, done_b = T_START, 0, 0

    def send(i, l):
        axis, cost = paths[l][i], sizes[i]
        if axis == 'c':
            cost = cost * 0.08
        lane = 'p' if axis == 'q' else axis
        link[lane] = max(now, link[lane]) + cost
        end = link[lane]
        if axis == 'q':
            link['m'] = max(end - cost, link['m']) + 2 * cost
            end = max(end, link['m'])
        arrive[i, l] = end + DELAY[axis]

    counts = False
    while True:
        ready = [k for k, v in arrive.items() if v <= now]
        first = paths[min(done_b, layers - 1)][1]
        if ready:
            if PRIO == 3:
                i, l = min(ready, key=lambda k: (-k[0], k[1]))
            elif PRIO == 0:
                i, l = min(ready)
            elif PRIO == 1:
                i, l = min(ready, key=lambda k: (k[1], k[0]))
            else:
                i, l = min(ready, key=lambda k: arrive[k])
            del arrive[i, l]
            now += T_STAGE[i]
            plan.append((i, l))
            if i < 9:
                send(i + 1, l)
        elif done_b < done_f and now >= T_COUNTS and (link[first] - now < AHEAD or not arrive):
            now += T_BWD
            if not counts:
                plan.append(('counts', 0))
                counts = True
            plan.append(('backward', done_b))
            send(0, done_b)
            done_b += 1
        elif done_f < layers:
            now += T_FWD
            plan.append(('forward', done_f))
            done_f += 1
        elif now < T_COUNTS:
            now = T_COUNTS
        elif arrive:
            now = min(arrive.values())
            if done_b < layers:
                now = min(now, max(link[first] - AHEAD + 0.01, now if now < min(arrive.values()) else 0))
                now = max(now, min(min(arrive.values()), link[first] - AHEAD + 0.01))
        else:
            return plan


def ring_kernel(dims, idx_hbm, u_hbm, w_hbm, e_hbm, d_hbm, out_ref, g_ref, loss_ref,
                idx_ref, u_all, w_all, e_buf, d_buf, wide, p_all, a_all, part, r0, r1, r2, r3, r4,
                cnt_src, cnt_buf, loss_src, loss_buf, loss_acc, pull_row,
                i_sem, u_sem, w_sem, e_sem, d_sem, *sems):
    layers, toks, num_exp, depth, top_k, group = dims
    send_sems, recv_sems = sems[:10], sems[10:20]
    cs, cv, ls, lv = sems[20:]
    landing = (r0, r1, r2, r3, r4)
    piece = depth // 16
    me = lax.axis_index('dp')
    bit = {axis: lax.rem(lax.div(me, step), 2) for axis, step in BITS.items()}
    peer = {axis: me + step * (1 - 2 * bit[axis]) for axis, step in BITS.items()}
    core = bit['c']
    tok_all = toks * group

    barrier = pltpu.get_barrier_semaphore()

    def greet(p, carry):
        pl.semaphore_signal(barrier, inc=1, device_id=(lax.rem(me + p, group),), device_id_type=MESH)
        return carry
    lax.fori_loop(1, group, greet, 0)

    def fetch(l):
        slot = lax.rem(l, SLOTS)
        return (pltpu.make_async_copy(u_hbm.at[l], u_all.at[l], u_sem.at[slot]),
                pltpu.make_async_copy(w_hbm.at[l], w_all.at[l], w_sem.at[slot]),
                pltpu.make_async_copy(e_hbm.at[l], e_buf.at[slot], e_sem.at[slot]),
                pltpu.make_async_copy(d_hbm.at[l], d_buf.at[slot], d_sem.at[slot]))

    get_idx = pltpu.make_async_copy(idx_hbm, idx_ref, i_sem)
    get_idx.start()
    for l in range(SLOTS):
        for copy in fetch(l):
            copy.start()
    loss_acc[...] = jnp.zeros_like(loss_acc)
    get_idx.wait()

    ids = [idx_ref[:, k, :] for k in range(top_k)]
    rows = []
    for e in range(num_exp):
        hit = jnp.where(ids[0] == e, 1.0, 0.0)
        for k in range(1, top_k):
            hit = hit + jnp.where(ids[k] == e, 1.0, 0.0)
        rows.append(hit)
    hits = jnp.concatenate(rows, axis=0).astype(jnp.bfloat16)
    cnt = lax.dot_general(jnp.ones((8, toks), jnp.bfloat16), hits, (((1,), (1,)), ((), ())),
                          preferred_element_type=jnp.float32)
    cnt_src[...] = cnt[0:1]
    cnt_buf[me] = cnt[0:1]

    def everyone(src, buf, ss, rs):
        def one(p, carry):
            pltpu.make_async_remote_copy(src_ref=src, dst_ref=buf.at[me], send_sem=ss, recv_sem=rs,
                                         device_id=(lax.rem(me + p, group),), device_id_type=MESH).start()
            return carry
        lax.fori_loop(1, group, one, 0)

    def drain(ref, sem):
        pltpu.make_async_copy(ref, ref, sem).wait()

    def forward(l):
        slot = lax.rem(l, SLOTS)
        for copy in fetch(l):
            copy.wait()
        logits = lax.dot_general(w_all[l], u_all[l], (((1,), (1,)), ((), ())), preferred_element_type=jnp.float32)
        accs = [[], []]
        tiles = depth // 128
        for tb in range(toks // 8):
            for t in range(8):
                tok = tb * 8 + t
                wide[pl.ds(tok * F_STRIDE, 2 * tiles), :] = (
                    e_buf[slot, pl.ds(tok * 2 * tiles, 2 * tiles), :].astype(jnp.float32))
            sums = [[None, None], [None, None]]
            for j in range(tiles):
                if j % 2 == 0:
                    dy = d_buf[slot, pl.ds((tb * tiles + j) * 8, 16), :].astype(jnp.float32)
                for k in range(2):
                    ev = wide[pl.ds(tb * 8 * F_STRIDE + 2 * j + k, 8, stride=F_STRIDE), :]
                    prod = ev * (dy[:8] if j % 2 == 0 else dy[8:])
                    old = sums[k][j % 2]
                    sums[k][j % 2] = prod if old is None else old + prod
            for k in range(2):
                accs[k].append(sums[k][0] + sums[k][1])

        @pl.when(l + SLOTS < layers)
        def _():
            for copy in fetch(l + SLOTS):
                copy.start()

        dots = jnp.sum(jnp.concatenate(accs[0] + accs[1], axis=0).T, axis=0, keepdims=True)
        dot0, dot1 = dots[:, :toks], dots[:, toks:]
        row_id = lax.broadcasted_iota(jnp.int32, (num_exp, toks), 0)
        pair = idx_ref[l]
        sel0 = row_id == pair[0:1]
        sel1 = row_id == pair[1:2]
        top = jnp.max(logits, axis=0, keepdims=True)
        ex = jnp.exp(logits - top)
        p_all[l] = ex / jnp.sum(ex, axis=0, keepdims=True)
        c0 = jnp.sum(jnp.where(sel0, logits, 0.0), axis=0, keepdims=True)
        c1 = jnp.sum(jnp.where(sel1, logits, 0.0), axis=0, keepdims=True)
        cm = jnp.maximum(c0, c1)
        x0, x1 = jnp.exp(c0 - cm), jnp.exp(c1 - cm)
        xs = x0 + x1
        g0, g1 = x0 / xs, x1 / xs
        inner = g0 * dot0 + g1 * dot1
        loss_acc[0:1, :] += inner
        scale = float(tok_all)
        dc0 = g0 * (scale * dot0 - scale * inner)
        dc1 = g1 * (scale * dot1 - scale * inner)
        a_all[l] = jnp.where(sel0, dc0, 0.0) + jnp.where(sel1, dc1, 0.0)

    def get_counts():
        drain(cnt_buf.at[pl.ds(0, group - 1)], cv)
        pull_row[...] = jnp.sum(cnt_buf[...], axis=0) * (AUX_COEF * num_exp / (top_k * tok_all))

    kept = {}
    for order in dict.fromkeys(ORDERS):
        offs = [0]
        for i, axis in enumerate(order):
            offs.append(offs[-1] + bit[axis] * (depth >> (i + 1)))
        kept[order] = offs

    def lanes(start, size):
        return pl.ds(start if isinstance(start, int) else pl.multiple_of(start, piece), size)

    def exchange(i, l):
        order = ORDERS[l]
        axis = ('c' + order + order[::-1] + 'c')[i]
        offs = kept[order]
        if i == 0:
            src, dst = part.at[l, 1 - core], r0.at[l]
        elif i < 5:
            size = depth >> i
            src = part.at[l, core, :, lanes(offs[i - 1] + (1 - bit[axis]) * size, size)]
            dst = landing[i].at[l]
        else:
            size = depth >> (9 - i)
            src = dst = out_ref.at[l, core, :, lanes(offs[9 - i], size)]
        return pltpu.make_async_remote_copy(src_ref=src, dst_ref=dst, send_sem=send_sems[i], recv_sem=recv_sems[i].at[l],
                                            device_id=(peer[axis],), device_id_type=MESH)

    def backward(l):
        at = lax.broadcasted_iota(jnp.int32, (num_exp, num_exp * layers), 1)
        row = lax.broadcasted_iota(jnp.int32, (num_exp, num_exp * layers), 0)
        pull = jnp.sum(jnp.where(at == layers * row + l, pull_row[...], 0.0), axis=1, keepdims=True)
        prob = p_all[l]
        inner = jnp.sum(prob * pull, axis=0, keepdims=True)
        loss_acc[1:2, :] += inner
        grad = (a_all[l] + prob * (pull - inner)).astype(jnp.bfloat16)
        g_ref[l] = grad
        dw = jnp.dot(grad, u_all[l], preferred_element_type=jnp.float32)
        part[l, 0] = dw[:8]
        part[l, 1] = dw[8:]
        exchange(0, l).start()
        if l == layers - 1:
            total = loss_acc[0:1, :] + loss_acc[1:2, :] * (1.0 / tok_all)
            mine = jnp.broadcast_to(jnp.sum(total, axis=1, keepdims=True), (1, 128))
            loss_src[...] = mine
            loss_buf[me] = mine
            everyone(loss_src, loss_buf, ls, lv)

    def arrived(i, l):
        order = ORDERS[l]
        offs = kept[order]
        if i < 5:
            exchange(i, l).wait_recv()
            got = landing[i]
            if i < 4:
                size = depth >> (i + 1)
                mine = bit[order[i]]
                for side in (1 - mine, mine):
                    here = lanes(offs[i] + side * size, size)
                    part[l, core, :, here] += got[l, :, lanes(side * size, size)]
                    if side is not mine:
                        exchange(i + 1, l).start()
            else:
                here = lanes(offs[4], piece)
                out_ref[l, core, :, here] = part[l, core, :, here] + got[l]
                exchange(5, l).start()
        else:
            exchange(i, l).wait_recv()
            if i < 9:
                exchange(i + 1, l).start()

    plan = plan_order(ORDERS)
    n_fwd = 0
    at = 0
    while at < len(plan):
        kind, l = plan[at]
        if kind == 'forward':
            stop = at
            while stop < len(plan) and plan[stop][0] == 'forward':
                stop += 1
            count = stop - at
            if n_fwd == 0:
                lax.fori_loop(0, GREET, lambda s, c: (forward(s), c)[1], 0)
                pl.semaphore_wait(barrier, group - 1)
                everyone(cnt_src, cnt_buf, cs, cv)
                lax.fori_loop(GREET, count, lambda s, c: (forward(s), c)[1], 0)
            else:
                lax.fori_loop(n_fwd, n_fwd + count, lambda s, c: (forward(s), c)[1], 0)
            n_fwd += count
            at = stop
            continue
        if kind == 'counts':
            get_counts()
        elif kind == 'backward':
            backward(l)
        else:
            arrived(kind, l)
        at += 1

    drain(loss_buf.at[pl.ds(0, group - 1)], lv)
    drain(loss_buf.at[pl.ds(0, group - 1)], ls)
    drain(cnt_buf.at[pl.ds(0, group - 1)], cs)
    for i in range(10):
        drain(landing[i if i < 5 else 9 - i], send_sems[i])
    loss_ref[...] = jnp.sum(loss_buf[...], axis=0)


def norm_kernel(per, g_ref, w_ref, dr_ref, dn_hbm, dr_hbm, buf, dn_sem, dr_sem):
    layers = g_ref.shape[0]
    move = pltpu.make_async_copy(dr_ref, dr_hbm, dr_sem)
    move.start()

    def put(b):
        return pltpu.make_async_copy(buf.at[pl.ds(b * per, per)], dn_hbm.at[pl.ds(b * per, per)], dn_sem.at[b])
    for b in range(layers // per):
        for l in range(b * per, b * per + per):
            buf[l] = lax.dot_general(g_ref[l], w_ref[l], (((0,), (0,)), ((), ())),
                                     preferred_element_type=jnp.float32).astype(jnp.bfloat16)
        put(b).start()
    for b in range(layers // per):
        put(b).wait()
    move.wait()


def solution(mesh):
    group = mesh.shape['dp']

    def local_step(u_norm, expert_idx, expert_out, d_out, w_router):
        layers, toks, depth = u_norm.shape
        num_exp = w_router.shape[2]
        top_k = expert_idx.shape[2]
        tiles = depth // 128
        idx_t = expert_idx.transpose(0, 2, 1)
        w_t = w_router.transpose(0, 2, 1)
        e_rows = expert_out.reshape(layers, toks, top_k, tiles, 128).transpose(0, 1, 3, 2, 4)
        e_rows = e_rows.reshape(layers, toks * tiles * top_k, 128)
        d_rows = d_out.reshape(layers, toks // 8, 8, tiles, 128).transpose(0, 1, 3, 2, 4)
        d_rows = d_rows.reshape(layers, toks * tiles, 128)
        f32, bf16 = jnp.float32, jnp.bfloat16
        dma = pltpu.SemaphoreType.DMA
        vmem = pl.BlockSpec(memory_space=pltpu.VMEM)
        hbm = pl.BlockSpec(memory_space=pltpu.HBM)
        dims = (layers, toks, num_exp, depth, top_k, group)
        scratch = [
            pltpu.VMEM((layers, top_k, toks), jnp.int32),
            pltpu.VMEM((layers, toks, depth), bf16), pltpu.VMEM((layers, num_exp, depth), bf16),
            pltpu.VMEM((SLOTS, toks * tiles * top_k, 128), bf16), pltpu.VMEM((SLOTS, toks * tiles, 128), bf16),
            pltpu.VMEM((toks * F_STRIDE, 128), f32),
            pltpu.VMEM((layers, num_exp, toks), f32), pltpu.VMEM((layers, num_exp, toks), f32),
            pltpu.VMEM((layers, 2, 8, depth), f32), pltpu.VMEM((layers, 8, depth), f32),
            pltpu.VMEM((layers, 8, depth // 2), f32), pltpu.VMEM((layers, 8, depth // 4), f32),
            pltpu.VMEM((layers, 8, depth // 8), f32), pltpu.VMEM((layers, 8, depth // 16), f32),
            pltpu.VMEM((1, num_exp * layers), f32), pltpu.VMEM((group, 1, num_exp * layers), f32),
            pltpu.VMEM((1, 128), f32), pltpu.VMEM((group, 1, 128), f32), pltpu.VMEM((8, toks), f32),
            pltpu.VMEM((1, num_exp * layers), f32),
            dma(()), dma((SLOTS,)), dma((SLOTS,)), dma((SLOTS,)), dma((SLOTS,)),
        ] + [dma(())] * 10 + [dma((layers,))] * 10 + [dma(())] * 4
        d_router, grads, loss = pl.pallas_call(
            functools.partial(ring_kernel, dims),
            out_shape=(pltpu.VMEM((layers, 2, 8, depth), f32), pltpu.VMEM((layers, num_exp, toks), bf16),
                       pltpu.VMEM((1, 128), f32)),
            in_specs=[hbm, hbm, hbm, hbm, hbm],
            out_specs=(vmem, vmem, vmem),
            scratch_shapes=scratch,
            compiler_params=pltpu.CompilerParams(collective_id=0, has_side_effects=True,
                                                 vmem_limit_bytes=48 * 1024 * 1024),
            name='ring',
        )(pltpu.with_memory_space_constraint(idx_t, pltpu.HBM), u_norm, pltpu.with_memory_space_constraint(w_t, pltpu.HBM), e_rows, d_rows)

        per = 2
        d_norm, d_router = pl.pallas_call(
            functools.partial(norm_kernel, per),
            out_shape=(jax.ShapeDtypeStruct((layers, toks, depth), bf16),
                       jax.ShapeDtypeStruct((layers, 2, 8, depth), f32)),
            in_specs=[vmem, vmem, vmem],
            out_specs=(hbm, hbm),
            scratch_shapes=[pltpu.VMEM((layers, toks, depth), bf16), dma((layers // per,)), dma(())],
            compiler_params=pltpu.CompilerParams(vmem_limit_bytes=20 * 1024 * 1024),
            name='norm',
        )(grads, w_t, d_router)
        d_router = d_router.reshape(layers, num_exp, depth).transpose(0, 2, 1)
        return loss[0, 0], d_router, d_norm

    tok_spec = P(None, 'dp', None)
    return jax.shard_map(local_step, mesh=mesh,
                         in_specs=(tok_spec, tok_spec, P(None, 'dp', None, None), tok_spec, P()),
                         out_specs=(P(), P(), tok_spec), check_vma=False)
```

```python
import functools

import jax
import jax.numpy as jnp
from jax import lax
from jax.experimental import pallas as pl
from jax.experimental.pallas import tpu as pltpu
from jax.sharding import PartitionSpec as P

AUX_COEF = 0.02
MESH = pl.DeviceIdType.MESH
F_STRIDE = 73
SLOTS = 6
GREET = 2
BITS = {'c': 1, 'x': 2, 'y': 4, 'p': 8, 'q': 16}
ORDERS = ('xpyq', 'ypxq') * 8
T_START, T_GREETED, T_COUNTS = 1.5, 7.5, 13.0
T_FWD, T_BWD, T_NORM = 0.72, 0.6, 0.35
T_STAGE = (0.1, 0.08, 0.06, 0.05, 0.05, 0.04, 0.04, 0.04, 0.04, 0.03)
DELAY = {'c': 1.53, 'x': 2.98, 'y': 2.98, 'p': 2.98, 'q': 3.4}
AHEAD = 3
PRIO = 3


def plan_order(orders):
    layers = len(orders)
    paths = ['c' + o + o[::-1] + 'c' for o in orders]
    sizes = [2.8 / 2 ** i for i in range(5)]
    sizes = sizes + sizes[::-1]
    link = dict.fromkeys('cxypm', 0.0)
    arrive, plan = {}, []
    now, done_f, done_b, done_n = T_START, 0, 0, 0

    def send(i, l):
        axis, cost = paths[l][i], sizes[i]
        if axis == 'c':
            cost = cost * 0.08
        lane = 'p' if axis == 'q' else axis
        link[lane] = max(now, link[lane]) + cost
        end = link[lane]
        if axis == 'q':
            link['m'] = max(end - cost, link['m']) + 2 * cost
            end = max(end, link['m'])
        arrive[i, l] = end + DELAY[axis]

    counts = False
    while True:
        ready = [k for k, v in arrive.items() if v <= now]
        first = paths[min(done_b, layers - 1)][1]
        if ready:
            if PRIO == 3:
                i, l = min(ready, key=lambda k: (-k[0], k[1]))
            elif PRIO == 0:
                i, l = min(ready)
            elif PRIO == 1:
                i, l = min(ready, key=lambda k: (k[1], k[0]))
            else:
                i, l = min(ready, key=lambda k: arrive[k])
            del arrive[i, l]
            now += T_STAGE[i]
            plan.append((i, l))
            if i < 9:
                send(i + 1, l)
        elif done_b < done_f and now >= T_COUNTS and (link[first] - now < AHEAD or not arrive):
            now += T_BWD
            if not counts:
                plan.append(('counts', 0))
                counts = True
            plan.append(('backward', done_b))
            send(0, done_b)
            done_b += 1
        elif done_f < layers:
            now += T_FWD
            plan.append(('forward', done_f))
            done_f += 1
            if done_f == GREET:
                now = max(now, T_GREETED)
        elif now < T_COUNTS:
            now = T_COUNTS
        elif done_n < done_b and (done_b == layers or min(arrive.values(), default=now + 9) > now + T_NORM):
            now += T_NORM
            plan.append(('norm', done_n))
            done_n += 1
        elif arrive:
            now = min(arrive.values())
            if done_b < layers:
                now = min(now, max(link[first] - AHEAD + 0.01, now if now < min(arrive.values()) else 0))
                now = max(now, min(min(arrive.values()), link[first] - AHEAD + 0.01))
        else:
            return plan


def ring_kernel(dims, idx_hbm, u_hbm, w_hbm, e_hbm, d_hbm, out_ref, dn_ref, loss_ref,
                idx_ref, u_all, w_all, e_buf, d_buf, wide, p_all, a_all, g_ref, part, r0, r1, r2, r3, r4,
                cnt_src, cnt_buf, loss_src, loss_buf, loss_acc, pull_row,
                i_sem, u_sem, w_sem, e_sem, d_sem, *sems):
    layers, toks, num_exp, depth, top_k, group = dims
    send_sems, recv_sems = sems[:10], sems[10:20]
    cs, cv, ls, lv = sems[20:]
    landing = (r0, r1, r2, r3, r4)
    piece = depth // 16
    me = lax.axis_index('dp')
    bit = {axis: lax.rem(lax.div(me, step), 2) for axis, step in BITS.items()}
    peer = {axis: me + step * (1 - 2 * bit[axis]) for axis, step in BITS.items()}
    core = bit['c']
    tok_all = toks * group

    barrier = pltpu.get_barrier_semaphore()

    def greet(p, carry):
        pl.semaphore_signal(barrier, inc=1, device_id=(lax.rem(me + p, group),), device_id_type=MESH)
        return carry
    lax.fori_loop(1, group, greet, 0)

    def fetch(l):
        slot = lax.rem(l, SLOTS)
        return (pltpu.make_async_copy(u_hbm.at[l], u_all.at[l], u_sem.at[slot]),
                pltpu.make_async_copy(w_hbm.at[l], w_all.at[l], w_sem.at[slot]),
                pltpu.make_async_copy(e_hbm.at[l], e_buf.at[slot], e_sem.at[slot]),
                pltpu.make_async_copy(d_hbm.at[l], d_buf.at[slot], d_sem.at[slot]))

    get_idx = pltpu.make_async_copy(idx_hbm, idx_ref, i_sem)
    get_idx.start()
    for l in range(SLOTS):
        for copy in fetch(l):
            copy.start()
    loss_acc[...] = jnp.zeros_like(loss_acc)
    get_idx.wait()

    ids = [idx_ref[:, k, :] for k in range(top_k)]
    rows = []
    for e in range(num_exp):
        hit = jnp.where(ids[0] == e, 1.0, 0.0)
        for k in range(1, top_k):
            hit = hit + jnp.where(ids[k] == e, 1.0, 0.0)
        rows.append(hit)
    hits = jnp.concatenate(rows, axis=0).astype(jnp.bfloat16)
    cnt = lax.dot_general(jnp.ones((8, toks), jnp.bfloat16), hits, (((1,), (1,)), ((), ())),
                          preferred_element_type=jnp.float32)
    cnt_src[...] = cnt[0:1]
    cnt_buf[me] = cnt[0:1]

    def everyone(src, buf, ss, rs):
        def one(p, carry):
            pltpu.make_async_remote_copy(src_ref=src, dst_ref=buf.at[me], send_sem=ss, recv_sem=rs,
                                         device_id=(lax.rem(me + p, group),), device_id_type=MESH).start()
            return carry
        lax.fori_loop(1, group, one, 0)

    def drain(ref, sem):
        pltpu.make_async_copy(ref, ref, sem).wait()

    def forward(l):
        slot = lax.rem(l, SLOTS)
        for copy in fetch(l):
            copy.wait()
        logits = lax.dot_general(w_all[l], u_all[l], (((1,), (1,)), ((), ())), preferred_element_type=jnp.float32)
        accs = [[], []]
        tiles = depth // 128
        for tb in range(toks // 8):
            for t in range(8):
                tok = tb * 8 + t
                wide[pl.ds(tok * F_STRIDE, 2 * tiles), :] = (
                    e_buf[slot, pl.ds(tok * 2 * tiles, 2 * tiles), :].astype(jnp.float32))
            sums = [[None, None], [None, None]]
            for j in range(tiles):
                if j % 2 == 0:
                    dy = d_buf[slot, pl.ds((tb * tiles + j) * 8, 16), :].astype(jnp.float32)
                for k in range(2):
                    ev = wide[pl.ds(tb * 8 * F_STRIDE + 2 * j + k, 8, stride=F_STRIDE), :]
                    prod = ev * (dy[:8] if j % 2 == 0 else dy[8:])
                    old = sums[k][j % 2]
                    sums[k][j % 2] = prod if old is None else old + prod
            for k in range(2):
                accs[k].append(sums[k][0] + sums[k][1])

        @pl.when(l + SLOTS < layers)
        def _():
            for copy in fetch(l + SLOTS):
                copy.start()

        dots = jnp.sum(jnp.concatenate(accs[0] + accs[1], axis=0).T, axis=0, keepdims=True)
        dot0, dot1 = dots[:, :toks], dots[:, toks:]
        row_id = lax.broadcasted_iota(jnp.int32, (num_exp, toks), 0)
        pair = idx_ref[l]
        sel0 = row_id == pair[0:1]
        sel1 = row_id == pair[1:2]
        top = jnp.max(logits, axis=0, keepdims=True)
        ex = jnp.exp(logits - top)
        p_all[l] = ex / jnp.sum(ex, axis=0, keepdims=True)
        c0 = jnp.sum(jnp.where(sel0, logits, 0.0), axis=0, keepdims=True)
        c1 = jnp.sum(jnp.where(sel1, logits, 0.0), axis=0, keepdims=True)
        cm = jnp.maximum(c0, c1)
        x0, x1 = jnp.exp(c0 - cm), jnp.exp(c1 - cm)
        xs = x0 + x1
        g0, g1 = x0 / xs, x1 / xs
        inner = g0 * dot0 + g1 * dot1
        loss_acc[0:1, :] += inner
        scale = float(tok_all)
        dc0 = g0 * (scale * dot0 - scale * inner)
        dc1 = g1 * (scale * dot1 - scale * inner)
        a_all[l] = jnp.where(sel0, dc0, 0.0) + jnp.where(sel1, dc1, 0.0)

    def get_counts():
        drain(cnt_buf.at[pl.ds(0, group - 1)], cv)
        pull_row[...] = jnp.sum(cnt_buf[...], axis=0) * (AUX_COEF * num_exp / (top_k * tok_all))

    kept = {}
    for order in dict.fromkeys(ORDERS):
        offs = [0]
        for i, axis in enumerate(order):
            offs.append(offs[-1] + bit[axis] * (depth >> (i + 1)))
        kept[order] = offs

    def lanes(start, size):
        return pl.ds(start if isinstance(start, int) else pl.multiple_of(start, piece), size)

    def exchange(i, l):
        order = ORDERS[l]
        axis = ('c' + order + order[::-1] + 'c')[i]
        offs = kept[order]
        if i == 0:
            src, dst = part.at[l, 1 - core], r0.at[l]
        elif i < 5:
            size = depth >> i
            src = part.at[l, core, :, lanes(offs[i - 1] + (1 - bit[axis]) * size, size)]
            dst = landing[i].at[l]
        else:
            size = depth >> (9 - i)
            src = dst = out_ref.at[l, core, :, lanes(offs[9 - i], size)]
        return pltpu.make_async_remote_copy(src_ref=src, dst_ref=dst, send_sem=send_sems[i], recv_sem=recv_sems[i].at[l],
                                            device_id=(peer[axis],), device_id_type=MESH)

    def backward(l):
        at = lax.broadcasted_iota(jnp.int32, (num_exp, num_exp * layers), 1)
        row = lax.broadcasted_iota(jnp.int32, (num_exp, num_exp * layers), 0)
        pull = jnp.sum(jnp.where(at == layers * row + l, pull_row[...], 0.0), axis=1, keepdims=True)
        prob = p_all[l]
        inner = jnp.sum(prob * pull, axis=0, keepdims=True)
        loss_acc[1:2, :] += inner
        grad = (a_all[l] + prob * (pull - inner)).astype(jnp.bfloat16)
        g_ref[l] = grad
        dw = jnp.dot(grad, u_all[l], preferred_element_type=jnp.float32)
        part[l, 0] = dw[:8]
        part[l, 1] = dw[8:]
        exchange(0, l).start()
        if l == layers - 1:
            total = loss_acc[0:1, :] + loss_acc[1:2, :] * (1.0 / tok_all)
            mine = jnp.broadcast_to(jnp.sum(total, axis=1, keepdims=True), (1, 128))
            loss_src[...] = mine
            loss_buf[me] = mine
            everyone(loss_src, loss_buf, ls, lv)

    def norm(l):
        dn_ref[l] = lax.dot_general(g_ref[l], w_all[l], (((0,), (0,)), ((), ())),
                                    preferred_element_type=jnp.float32).astype(jnp.bfloat16)

    def arrived(i, l):
        order = ORDERS[l]
        offs = kept[order]
        if i < 5:
            exchange(i, l).wait_recv()
            got = landing[i]
            if i < 4:
                size = depth >> (i + 1)
                mine = bit[order[i]]
                for side in (1 - mine, mine):
                    here = lanes(offs[i] + side * size, size)
                    part[l, core, :, here] += got[l, :, lanes(side * size, size)]
                    if side is not mine:
                        exchange(i + 1, l).start()
            else:
                here = lanes(offs[4], piece)
                out_ref[l, core, :, here] = part[l, core, :, here] + got[l]
                exchange(5, l).start()
        else:
            exchange(i, l).wait_recv()
            if i < 9:
                exchange(i + 1, l).start()

    plan = plan_order(ORDERS)
    n_fwd = 0
    at = 0
    while at < len(plan):
        kind, l = plan[at]
        if kind == 'forward':
            stop = at
            while stop < len(plan) and plan[stop][0] == 'forward':
                stop += 1
            count = stop - at
            if n_fwd == 0:
                lax.fori_loop(0, GREET, lambda s, c: (forward(s), c)[1], 0)
                pl.semaphore_wait(barrier, group - 1)
                everyone(cnt_src, cnt_buf, cs, cv)
                lax.fori_loop(GREET, count, lambda s, c: (forward(s), c)[1], 0)
            else:
                lax.fori_loop(n_fwd, n_fwd + count, lambda s, c: (forward(s), c)[1], 0)
            n_fwd += count
            at = stop
            continue
        if kind == 'counts':
            get_counts()
        elif kind == 'backward':
            backward(l)
        elif kind == 'norm':
            norm(l)
        else:
            arrived(kind, l)
        at += 1

    drain(loss_buf.at[pl.ds(0, group - 1)], lv)
    drain(loss_buf.at[pl.ds(0, group - 1)], ls)
    drain(cnt_buf.at[pl.ds(0, group - 1)], cs)
    for i in range(10):
        drain(landing[i if i < 5 else 9 - i], send_sems[i])
    loss_ref[...] = jnp.sum(loss_buf[...], axis=0)


def put_kernel(parts, dn_ref, dr_ref, dn_hbm, dr_hbm, sem):
    layers = dn_ref.shape[0]
    per = layers // parts
    copies = []
    for b in range(parts):
        at = pl.ds(b * per, per)
        copies.append(pltpu.make_async_copy(dn_ref.at[at], dn_hbm.at[at], sem.at[2 * b]))
        copies.append(pltpu.make_async_copy(dr_ref.at[at], dr_hbm.at[at], sem.at[2 * b + 1]))
    for copy in copies:
        copy.start()
    for copy in copies:
        copy.wait()


def solution(mesh):
    group = mesh.shape['dp']

    def local_step(u_norm, expert_idx, expert_out, d_out, w_router):
        layers, toks, depth = u_norm.shape
        num_exp = w_router.shape[2]
        top_k = expert_idx.shape[2]
        tiles = depth // 128
        idx_t = expert_idx.transpose(0, 2, 1)
        w_t = w_router.transpose(0, 2, 1)
        e_rows = expert_out.reshape(layers, toks, top_k, tiles, 128).transpose(0, 1, 3, 2, 4)
        e_rows = e_rows.reshape(layers, toks * tiles * top_k, 128)
        d_rows = d_out.reshape(layers, toks // 8, 8, tiles, 128).transpose(0, 1, 3, 2, 4)
        d_rows = d_rows.reshape(layers, toks * tiles, 128)
        f32, bf16 = jnp.float32, jnp.bfloat16
        dma = pltpu.SemaphoreType.DMA
        vmem = pl.BlockSpec(memory_space=pltpu.VMEM)
        hbm = pl.BlockSpec(memory_space=pltpu.HBM)
        dims = (layers, toks, num_exp, depth, top_k, group)
        scratch = [
            pltpu.VMEM((layers, top_k, toks), jnp.int32),
            pltpu.VMEM((layers, toks, depth), bf16), pltpu.VMEM((layers, num_exp, depth), bf16),
            pltpu.VMEM((SLOTS, toks * tiles * top_k, 128), bf16), pltpu.VMEM((SLOTS, toks * tiles, 128), bf16),
            pltpu.VMEM((toks * F_STRIDE, 128), f32),
            pltpu.VMEM((layers, num_exp, toks), f32), pltpu.VMEM((layers, num_exp, toks), f32),
            pltpu.VMEM((layers, num_exp, toks), bf16),
            pltpu.VMEM((layers, 2, 8, depth), f32), pltpu.VMEM((layers, 8, depth), f32),
            pltpu.VMEM((layers, 8, depth // 2), f32), pltpu.VMEM((layers, 8, depth // 4), f32),
            pltpu.VMEM((layers, 8, depth // 8), f32), pltpu.VMEM((layers, 8, depth // 16), f32),
            pltpu.VMEM((1, num_exp * layers), f32), pltpu.VMEM((group, 1, num_exp * layers), f32),
            pltpu.VMEM((1, 128), f32), pltpu.VMEM((group, 1, 128), f32), pltpu.VMEM((8, toks), f32),
            pltpu.VMEM((1, num_exp * layers), f32),
            dma(()), dma((SLOTS,)), dma((SLOTS,)), dma((SLOTS,)), dma((SLOTS,)),
        ] + [dma(())] * 10 + [dma((layers,))] * 10 + [dma(())] * 4
        d_router, d_norm, loss = pl.pallas_call(
            functools.partial(ring_kernel, dims),
            out_shape=(pltpu.VMEM((layers, 2, 8, depth), f32), pltpu.VMEM((layers, toks, depth), bf16),
                       pltpu.VMEM((1, 128), f32)),
            in_specs=[hbm, hbm, hbm, hbm, hbm],
            out_specs=(vmem, vmem, vmem),
            scratch_shapes=scratch,
            compiler_params=pltpu.CompilerParams(collective_id=0, has_side_effects=True,
                                                 vmem_limit_bytes=40 * 1024 * 1024),
            name='ring',
        )(pltpu.with_memory_space_constraint(idx_t, pltpu.HBM), u_norm, pltpu.with_memory_space_constraint(w_t, pltpu.HBM), e_rows, d_rows)

        parts = 4
        d_norm, d_router = pl.pallas_call(
            functools.partial(put_kernel, parts),
            out_shape=(jax.ShapeDtypeStruct((layers, toks, depth), bf16),
                       jax.ShapeDtypeStruct((layers, 2, 8, depth), f32)),
            in_specs=[vmem, vmem],
            out_specs=(hbm, hbm),
            scratch_shapes=[dma((2 * parts,))],
            compiler_params=pltpu.CompilerParams(vmem_limit_bytes=1024 * 1024),
            name='put',
        )(d_norm, d_router)
        d_router = d_router.reshape(layers, num_exp, depth).transpose(0, 2, 1)
        return loss[0, 0], d_router, d_norm

    tok_spec = P(None, 'dp', None)
    return jax.shard_map(local_step, mesh=mesh,
                         in_specs=(tok_spec, tok_spec, P(None, 'dp', None, None), tok_spec, P()),
                         out_specs=(P(), P(), tok_spec), check_vma=False)
```

```python
import functools

import jax
import jax.numpy as jnp
from jax import lax
from jax.experimental import pallas as pl
from jax.experimental.pallas import tpu as pltpu
from jax.sharding import PartitionSpec as P

AUX_COEF = 0.02
MESH = pl.DeviceIdType.MESH
F_STRIDE = 73
SLOTS = 6
GREET = 2
BITS = {'c': 1, 'x': 2, 'y': 4, 'p': 8, 'q': 16}
ORDERS = ('xypq', 'yxpq', 'pqxy', 'xypq', 'yxpq') * 3 + ('xypq',)
T_START, T_GREETED, T_COUNTS = 1.5, 7.5, 13.0
T_FWD, T_BWD, T_NORM = 0.72, 0.6, 0.35
T_STAGE = (0.1, 0.08, 0.06, 0.05, 0.05, 0.04, 0.04, 0.04, 0.04, 0.03)
DELAY = {'c': 1.53, 'x': 2.98, 'y': 2.98, 'p': 2.98, 'q': 3.4}
AHEAD = 2.5
PRIO = 3


def plan_order(orders):
    layers = len(orders)
    paths = ['c' + o + o[::-1] + 'c' for o in orders]
    sizes = [2.8 / 2 ** i for i in range(5)]
    sizes = sizes + sizes[::-1]
    link = dict.fromkeys('cxypm', 0.0)
    arrive, early, plan = {}, {}, []
    now, done_f, done_b, done_n = T_START, 0, 0, 0

    def occupy(i, l, share):
        axis = paths[l][i]
        cost = sizes[i] * share * (0.08 if axis == 'c' else 1.0)
        lane = 'p' if axis == 'q' else axis
        link[lane] = max(now, link[lane]) + cost
        end = link[lane]
        if axis == 'q':
            link['m'] = max(end - cost, link['m']) + 2 * cost
            end = max(end, link['m'])
        return end + DELAY[axis]

    def send(i, l):
        end = occupy(i, l, 1.0 if i < 6 else 0.5)
        arrive[i, l] = max(end, early.pop((i, l), 0.0))
        if 5 <= i < 9:
            early[i + 1, l] = occupy(i + 1, l, 0.5)

    counts = False
    while True:
        ready = [k for k, v in arrive.items() if v <= now]
        first = paths[min(done_b, layers - 1)][1]
        if ready:
            if PRIO == 3:
                i, l = min(ready, key=lambda k: (-k[0], k[1]))
            elif PRIO == 0:
                i, l = min(ready)
            elif PRIO == 1:
                i, l = min(ready, key=lambda k: (k[1], k[0]))
            else:
                i, l = min(ready, key=lambda k: arrive[k])
            del arrive[i, l]
            now += T_STAGE[i]
            plan.append((i, l))
            if i < 9:
                send(i + 1, l)
        elif done_b < done_f and now >= T_COUNTS and (link[first] - now < AHEAD or not arrive):
            now += T_BWD
            if not counts:
                plan.append(('counts', 0))
                counts = True
            plan.append(('backward', done_b))
            send(0, done_b)
            done_b += 1
        elif done_f < layers:
            now += T_FWD
            plan.append(('forward', done_f))
            done_f += 1
            if done_f == GREET:
                now = max(now, T_GREETED)
        elif now < T_COUNTS:
            now = T_COUNTS
        elif done_n < done_b and (done_b == layers or min(arrive.values(), default=now + 9) > now + T_NORM):
            now += T_NORM
            plan.append(('norm', done_n))
            done_n += 1
        elif arrive:
            now = min(arrive.values())
            if done_b < layers:
                now = min(now, max(link[first] - AHEAD + 0.01, now if now < min(arrive.values()) else 0))
                now = max(now, min(min(arrive.values()), link[first] - AHEAD + 0.01))
        else:
            return plan


def ring_kernel(dims, idx_hbm, u_hbm, w_hbm, e_hbm, d_hbm, out_ref, dn_ref, loss_ref,
                idx_ref, u_all, w_all, e_buf, d_buf, wide, p_all, a_all, g_ref, part, r0, r1, r2, r3, r4,
                cnt_src, cnt_buf, loss_src, loss_buf, loss_acc, pull_row,
                i_sem, u_sem, w_sem, e_sem, d_sem, *sems):
    layers, toks, num_exp, depth, top_k, group = dims
    send_sems, recv_sems = sems[:10], sems[10:20]
    cs, cv, ls, lv = sems[20:]
    landing = (r0, r1, r2, r3, r4)
    piece = depth // 16
    me = lax.axis_index('dp')
    bit = {axis: lax.rem(lax.div(me, step), 2) for axis, step in BITS.items()}
    peer = {axis: me + step * (1 - 2 * bit[axis]) for axis, step in BITS.items()}
    core = bit['c']
    tok_all = toks * group

    barrier = pltpu.get_barrier_semaphore()

    def greet(p, carry):
        pl.semaphore_signal(barrier, inc=1, device_id=(lax.rem(me + p, group),), device_id_type=MESH)
        return carry
    lax.fori_loop(1, group, greet, 0)

    def fetch(l):
        slot = lax.rem(l, SLOTS)
        return (pltpu.make_async_copy(u_hbm.at[l], u_all.at[l], u_sem.at[slot]),
                pltpu.make_async_copy(w_hbm.at[l], w_all.at[l], w_sem.at[slot]),
                pltpu.make_async_copy(e_hbm.at[l], e_buf.at[slot], e_sem.at[slot]),
                pltpu.make_async_copy(d_hbm.at[l], d_buf.at[slot], d_sem.at[slot]))

    get_idx = pltpu.make_async_copy(idx_hbm, idx_ref, i_sem)
    get_idx.start()
    for l in range(SLOTS):
        for copy in fetch(l):
            copy.start()
    loss_acc[...] = jnp.zeros_like(loss_acc)
    get_idx.wait()

    ids = [idx_ref[:, k, :] for k in range(top_k)]
    rows = []
    for e in range(num_exp):
        hit = jnp.where(ids[0] == e, 1.0, 0.0)
        for k in range(1, top_k):
            hit = hit + jnp.where(ids[k] == e, 1.0, 0.0)
        rows.append(hit)
    hits = jnp.concatenate(rows, axis=0).astype(jnp.bfloat16)
    cnt = lax.dot_general(jnp.ones((8, toks), jnp.bfloat16), hits, (((1,), (1,)), ((), ())),
                          preferred_element_type=jnp.float32)
    cnt_src[...] = cnt[0:1]
    cnt_buf[me] = cnt[0:1]

    def everyone(src, buf, ss, rs):
        def one(p, carry):
            pltpu.make_async_remote_copy(src_ref=src, dst_ref=buf.at[me], send_sem=ss, recv_sem=rs,
                                         device_id=(lax.rem(me + p, group),), device_id_type=MESH).start()
            return carry
        lax.fori_loop(1, group, one, 0)

    def drain(ref, sem):
        pltpu.make_async_copy(ref, ref, sem).wait()

    def forward(l):
        slot = lax.rem(l, SLOTS)
        for copy in fetch(l):
            copy.wait()
        logits = lax.dot_general(w_all[l], u_all[l], (((1,), (1,)), ((), ())), preferred_element_type=jnp.float32)
        accs = [[], []]
        tiles = depth // 128
        for tb in range(toks // 8):
            for t in range(8):
                tok = tb * 8 + t
                wide[pl.ds(tok * F_STRIDE, 2 * tiles), :] = (
                    e_buf[slot, pl.ds(tok * 2 * tiles, 2 * tiles), :].astype(jnp.float32))
            sums = [[None, None], [None, None]]
            for j in range(tiles):
                if j % 2 == 0:
                    dy = d_buf[slot, pl.ds((tb * tiles + j) * 8, 16), :].astype(jnp.float32)
                for k in range(2):
                    ev = wide[pl.ds(tb * 8 * F_STRIDE + 2 * j + k, 8, stride=F_STRIDE), :]
                    prod = ev * (dy[:8] if j % 2 == 0 else dy[8:])
                    old = sums[k][j % 2]
                    sums[k][j % 2] = prod if old is None else old + prod
            for k in range(2):
                accs[k].append(sums[k][0] + sums[k][1])

        @pl.when(l + SLOTS < layers)
        def _():
            for copy in fetch(l + SLOTS):
                copy.start()

        dots = jnp.sum(jnp.concatenate(accs[0] + accs[1], axis=0).T, axis=0, keepdims=True)
        dot0, dot1 = dots[:, :toks], dots[:, toks:]
        row_id = lax.broadcasted_iota(jnp.int32, (num_exp, toks), 0)
        pair = idx_ref[l]
        sel0 = row_id == pair[0:1]
        sel1 = row_id == pair[1:2]
        top = jnp.max(logits, axis=0, keepdims=True)
        ex = jnp.exp(logits - top)
        p_all[l] = ex / jnp.sum(ex, axis=0, keepdims=True)
        c0 = jnp.sum(jnp.where(sel0, logits, 0.0), axis=0, keepdims=True)
        c1 = jnp.sum(jnp.where(sel1, logits, 0.0), axis=0, keepdims=True)
        cm = jnp.maximum(c0, c1)
        x0, x1 = jnp.exp(c0 - cm), jnp.exp(c1 - cm)
        xs = x0 + x1
        g0, g1 = x0 / xs, x1 / xs
        inner = g0 * dot0 + g1 * dot1
        loss_acc[0:1, :] += inner
        scale = float(tok_all)
        dc0 = g0 * (scale * dot0 - scale * inner)
        dc1 = g1 * (scale * dot1 - scale * inner)
        a_all[l] = jnp.where(sel0, dc0, 0.0) + jnp.where(sel1, dc1, 0.0)

    def get_counts():
        drain(cnt_buf.at[pl.ds(0, group - 1)], cv)
        pull_row[...] = jnp.sum(cnt_buf[...], axis=0) * (AUX_COEF * num_exp / (top_k * tok_all))

    kept = {}
    for order in dict.fromkeys(ORDERS):
        offs = [0]
        for i, axis in enumerate(order):
            offs.append(offs[-1] + bit[axis] * (depth >> (i + 1)))
        kept[order] = offs

    def lanes(start, size):
        return pl.ds(start if isinstance(start, int) else pl.multiple_of(start, piece), size)

    def remote(i, l, src, dst):
        axis = ('c' + ORDERS[l] + ORDERS[l][::-1] + 'c')[i]
        return pltpu.make_async_remote_copy(src_ref=src, dst_ref=dst, send_sem=send_sems[i], recv_sem=recv_sems[i].at[l],
                                            device_id=(peer[axis],), device_id_type=MESH)

    def scatter(i, l):
        offs = kept[ORDERS[l]]
        if i == 0:
            return remote(i, l, part.at[l, 1 - core], r0.at[l])
        size = depth >> i
        src = part.at[l, core, :, lanes(offs[i - 1] + (1 - bit[ORDERS[l][i - 1]]) * size, size)]
        return remote(i, l, src, landing[i].at[l])

    def gather(i, l):
        order = ORDERS[l]
        offs = kept[order]
        level = 9 - i
        size = depth >> level
        if i == 5:
            parts = [(i, offs[level], size)]
        else:
            parts = [(i, offs[level] + (1 - bit[order[level]]) * (size // 2), size // 2)]
        if i < 9:
            parts.append((i + 1, offs[level], size))
        for step, start, width in parts:
            ref = out_ref.at[l, core, :, lanes(start, width)]
            remote(step, l, ref, ref).start()

    def backward(l):
        at = lax.broadcasted_iota(jnp.int32, (num_exp, num_exp * layers), 1)
        row = lax.broadcasted_iota(jnp.int32, (num_exp, num_exp * layers), 0)
        pull = jnp.sum(jnp.where(at == layers * row + l, pull_row[...], 0.0), axis=1, keepdims=True)
        prob = p_all[l]
        inner = jnp.sum(prob * pull, axis=0, keepdims=True)
        loss_acc[1:2, :] += inner
        grad = (a_all[l] + prob * (pull - inner)).astype(jnp.bfloat16)
        g_ref[l] = grad
        dw = jnp.dot(grad, u_all[l], preferred_element_type=jnp.float32)
        part[l, 0] = dw[:8]
        part[l, 1] = dw[8:]
        scatter(0, l).start()
        if l == layers - 1:
            total = loss_acc[0:1, :] + loss_acc[1:2, :] * (1.0 / tok_all)
            mine = jnp.broadcast_to(jnp.sum(total, axis=1, keepdims=True), (1, 128))
            loss_src[...] = mine
            loss_buf[me] = mine
            everyone(loss_src, loss_buf, ls, lv)

    def norm(l):
        dn_ref[l] = lax.dot_general(g_ref[l], w_all[l], (((0,), (0,)), ((), ())),
                                    preferred_element_type=jnp.float32).astype(jnp.bfloat16)

    def arrived(i, l):
        order = ORDERS[l]
        offs = kept[order]
        if i < 5:
            scatter(i, l).wait_recv()
            got = landing[i]
            if i < 4:
                size = depth >> (i + 1)
                mine = bit[order[i]]
                for side in (1 - mine, mine):
                    here = lanes(offs[i] + side * size, size)
                    part[l, core, :, here] += got[l, :, lanes(side * size, size)]
                    if side is not mine:
                        scatter(i + 1, l).start()
            else:
                here = lanes(offs[4], piece)
                out_ref[l, core, :, here] = part[l, core, :, here] + got[l]
                gather(5, l)
        else:
            drain(landing[9 - i].at[l], recv_sems[i].at[l])
            if i < 9:
                gather(i + 1, l)

    plan = plan_order(ORDERS)
    n_fwd = 0
    at = 0
    while at < len(plan):
        kind, l = plan[at]
        if kind == 'forward':
            stop = at
            while stop < len(plan) and plan[stop][0] == 'forward':
                stop += 1
            count = stop - at
            if n_fwd == 0:
                lax.fori_loop(0, GREET, lambda s, c: (forward(s), c)[1], 0)
                pl.semaphore_wait(barrier, group - 1)
                everyone(cnt_src, cnt_buf, cs, cv)
                lax.fori_loop(GREET, count, lambda s, c: (forward(s), c)[1], 0)
            else:
                lax.fori_loop(n_fwd, n_fwd + count, lambda s, c: (forward(s), c)[1], 0)
            n_fwd += count
            at = stop
            continue
        if kind == 'counts':
            get_counts()
        elif kind == 'backward':
            backward(l)
        elif kind == 'norm':
            norm(l)
        else:
            arrived(kind, l)
        at += 1

    drain(loss_buf.at[pl.ds(0, group - 1)], lv)
    drain(loss_buf.at[pl.ds(0, group - 1)], ls)
    drain(cnt_buf.at[pl.ds(0, group - 1)], cs)
    for i in range(10):
        drain(landing[i if i < 5 else 9 - i], send_sems[i])
    loss_ref[...] = jnp.sum(loss_buf[...], axis=0)


def put_kernel(parts, dn_ref, dr_ref, dn_hbm, dr_hbm, sem):
    layers = dn_ref.shape[0]
    per = layers // parts
    copies = []
    for b in range(parts):
        at = pl.ds(b * per, per)
        copies.append(pltpu.make_async_copy(dn_ref.at[at], dn_hbm.at[at], sem.at[2 * b]))
        copies.append(pltpu.make_async_copy(dr_ref.at[at], dr_hbm.at[at], sem.at[2 * b + 1]))
    for copy in copies:
        copy.start()
    for copy in copies:
        copy.wait()


def solution(mesh):
    group = mesh.shape['dp']

    def local_step(u_norm, expert_idx, expert_out, d_out, w_router):
        layers, toks, depth = u_norm.shape
        num_exp = w_router.shape[2]
        top_k = expert_idx.shape[2]
        tiles = depth // 128
        idx_t = expert_idx.transpose(0, 2, 1)
        w_t = w_router.transpose(0, 2, 1)
        e_rows = expert_out.reshape(layers, toks, top_k, tiles, 128).transpose(0, 1, 3, 2, 4)
        e_rows = e_rows.reshape(layers, toks * tiles * top_k, 128)
        d_rows = d_out.reshape(layers, toks // 8, 8, tiles, 128).transpose(0, 1, 3, 2, 4)
        d_rows = d_rows.reshape(layers, toks * tiles, 128)
        f32, bf16 = jnp.float32, jnp.bfloat16
        dma = pltpu.SemaphoreType.DMA
        vmem = pl.BlockSpec(memory_space=pltpu.VMEM)
        hbm = pl.BlockSpec(memory_space=pltpu.HBM)
        dims = (layers, toks, num_exp, depth, top_k, group)
        scratch = [
            pltpu.VMEM((layers, top_k, toks), jnp.int32),
            pltpu.VMEM((layers, toks, depth), bf16), pltpu.VMEM((layers, num_exp, depth), bf16),
            pltpu.VMEM((SLOTS, toks * tiles * top_k, 128), bf16), pltpu.VMEM((SLOTS, toks * tiles, 128), bf16),
            pltpu.VMEM((toks * F_STRIDE, 128), f32),
            pltpu.VMEM((layers, num_exp, toks), f32), pltpu.VMEM((layers, num_exp, toks), f32),
            pltpu.VMEM((layers, num_exp, toks), bf16),
            pltpu.VMEM((layers, 2, 8, depth), f32), pltpu.VMEM((layers, 8, depth), f32),
            pltpu.VMEM((layers, 8, depth // 2), f32), pltpu.VMEM((layers, 8, depth // 4), f32),
            pltpu.VMEM((layers, 8, depth // 8), f32), pltpu.VMEM((layers, 8, depth // 16), f32),
            pltpu.VMEM((1, num_exp * layers), f32), pltpu.VMEM((group, 1, num_exp * layers), f32),
            pltpu.VMEM((1, 128), f32), pltpu.VMEM((group, 1, 128), f32), pltpu.VMEM((8, toks), f32),
            pltpu.VMEM((1, num_exp * layers), f32),
            dma(()), dma((SLOTS,)), dma((SLOTS,)), dma((SLOTS,)), dma((SLOTS,)),
        ] + [dma(())] * 10 + [dma((layers,))] * 10 + [dma(())] * 4
        d_router, d_norm, loss = pl.pallas_call(
            functools.partial(ring_kernel, dims),
            out_shape=(pltpu.VMEM((layers, 2, 8, depth), f32), pltpu.VMEM((layers, toks, depth), bf16),
                       pltpu.VMEM((1, 128), f32)),
            in_specs=[hbm, hbm, hbm, hbm, hbm],
            out_specs=(vmem, vmem, vmem),
            scratch_shapes=scratch,
            compiler_params=pltpu.CompilerParams(collective_id=0, has_side_effects=True,
                                                 vmem_limit_bytes=40 * 1024 * 1024),
            name='ring',
        )(pltpu.with_memory_space_constraint(idx_t, pltpu.HBM), u_norm, pltpu.with_memory_space_constraint(w_t, pltpu.HBM), e_rows, d_rows)

        parts = 4
        d_norm, d_router = pl.pallas_call(
            functools.partial(put_kernel, parts),
            out_shape=(jax.ShapeDtypeStruct((layers, toks, depth), bf16),
                       jax.ShapeDtypeStruct((layers, 2, 8, depth), f32)),
            in_specs=[vmem, vmem],
            out_specs=(hbm, hbm),
            scratch_shapes=[dma((2 * parts,))],
            compiler_params=pltpu.CompilerParams(vmem_limit_bytes=1024 * 1024),
            name='put',
        )(d_norm, d_router)
        d_router = d_router.reshape(layers, num_exp, depth).transpose(0, 2, 1)
        return loss[0, 0], d_router, d_norm

    tok_spec = P(None, 'dp', None)
    return jax.shard_map(local_step, mesh=mesh,
                         in_specs=(tok_spec, tok_spec, P(None, 'dp', None, None), tok_spec, P()),
                         out_specs=(P(), P(), tok_spec), check_vma=False)
```
